32 devices in a mesh: ctx: 16 (over z, y, x), head: 2 (over core).
Axes of the slice: x: 2, y: 2, z: 4, core: 2. Of those that a mesh axis runs over, the one named last changes fastest.
Arguments:
- queries: bfloat16 [4096, 4096], P('ctx', 'head'), may hold values from -200 to 200
- span_keys: bfloat16 [4096, 4096], P('ctx', 'head'), may hold values from -6 to 6
- span_values: bfloat16 [4096, 4096], P('ctx', 'head'), may hold values from -96 to 96
- cache_keys: bfloat16 [16384, 4096], P('ctx', 'head'), may hold values from -6 to 6
- cache_values: bfloat16 [16384, 4096], P('ctx', 'head'), may hold values from -96 to 96
- land_keys: bfloat16 [256, 4096], P('ctx', 'head'), may hold values from -4.5 to 4.5
- land_values: bfloat16 [256, 4096], P('ctx', 'head'), may hold values from -96 to 96
- out_weight: bfloat16 [4096, 4096], P('head', 'ctx'), may hold values from -0.09375 to 0.09375
- selection: int32 [64, 32, 4], P('ctx', 'head'), may hold values from 0 to 255, as said below
Outputs:
- projected: bfloat16 [4096, 4096], P('ctx', 'head')
The draws below stay inside these ranges and needn't reach their ends.
Inputs may be any that keep to these rules, and one draw needn't show every extreme that they name: `selection`: the 4 blocks of one query group and head are distinct. Count block b as owned by ctx index b // 16. Over all groups and heads of one device (one index of ctx and one of head), the selections within one owner's blocks number at most 32 and form at most 8 distinct pairs of block and head; some owner receives exactly that many of both from every device.
All inputs are finite; a program needn't handle non-finite values.
Results may differ from the reference program's by a relative error of at most 0.015.
Values may be sent and summed in bfloat16 or wider, within the bound.
No kernel may reach another device: no remote copies, remote signals or barrier semaphores. Data moves between devices by JAX's collectives and lax.ppermute only.
A program may use at most 128 MiB of HBM per device.

```python
import math
import jax
import jax.numpy as jnp
from jax import lax

D = 4096
HEADS = 32
DH = 128
BLOCK = 64
TOPB = 4
BLK_DEV = 16
G_DEV = 4
SPAN = 4096
NCTX = 16384
NBLK = 256
NGROUP = 64
N_CTX = 16
N_HEAD = 2


def shared_fields(key):
    base_key = jax.random.fold_in(key, 4099)
    land_key = jax.random.fold_in(base_key, 0)
    query_key = jax.random.fold_in(base_key, 1)
    span_key = jax.random.fold_in(base_key, 3)
    full_width = HEADS * DH
    landmark = jnp.clip(jax.random.normal(land_key, (NBLK, full_width), jnp.float32), -4.5, 4.5)
    query_rows = jnp.clip(jax.random.normal(query_key, (SPAN, full_width), jnp.float32), -6.0, 6.0)
    span_rows = jnp.clip(jax.random.normal(span_key, (SPAN, full_width), jnp.float32), -6.0, 6.0)
    return (query_rows, landmark, span_rows)


def draw_queries(key, part):
    query_rows, landmark, span_rows = shared_fields(key)
    return query_rows.astype(jnp.bfloat16)


def draw_land_keys(key, part):
    query_rows, landmark, span_rows = shared_fields(key)
    return landmark.astype(jnp.bfloat16)


def draw_span_keys(key, part):
    query_rows, landmark, span_rows = shared_fields(key)
    return span_rows.astype(jnp.bfloat16)


def device_picks(subkey, popular):
    head_dev = HEADS // N_HEAD
    candidate_count = 2 * TOPB
    slot_most = (head_dev * candidate_count + N_CTX - 1) // N_CTX
    pool_size = N_CTX * slot_most
    prio_key, owner_key, first_key, rest_key, group_key = jax.random.split(subkey, 5)
    pool_owner = jnp.arange(pool_size, dtype=jnp.int32) // slot_most
    pool_rank = jnp.arange(pool_size, dtype=jnp.int32) % slot_most
    priority = jax.random.randint(prio_key, (pool_size,), 0, 4096, dtype=jnp.int32)
    priority = priority + pool_owner * 4096 // max(N_CTX - 1, 1)
    priority = priority + jnp.where(pool_owner == popular, 1 << 16, 0).astype(jnp.int32)
    priority = priority * pool_size + jnp.arange(pool_size, dtype=jnp.int32)
    chosen = lax.top_k(priority, head_dev * candidate_count)[1].astype(jnp.int32)
    leading = jax.random.permutation(first_key, chosen[:head_dev])
    trailing = jax.random.permutation(rest_key, chosen[head_dev:]).reshape(head_dev, candidate_count - 1)
    slot_table = jnp.concatenate([leading[:, None], trailing], axis=1)
    owner_base = jax.random.randint(owner_key, (N_CTX,), 0, BLK_DEV, dtype=jnp.int32)
    cand_owner = pool_owner[slot_table]
    local_block = (owner_base[cand_owner] + pool_rank[slot_table]) % BLK_DEV
    candidates = cand_owner * BLK_DEV + local_block
    group_keys = jax.random.split(group_key, G_DEV * head_dev)
    head_list = jnp.tile(jnp.arange(head_dev, dtype=jnp.int32), G_DEV)

    def one_group(pick_key, head_index):
        order_key, shuffle_key = jax.random.split(pick_key)
        others = jax.random.permutation(order_key, candidate_count - 1)[:TOPB - 1].astype(jnp.int32) + 1
        picked = jnp.concatenate([jnp.zeros((1,), jnp.int32), others])
        picked = jax.random.permutation(shuffle_key, picked)
        return candidates[head_index, picked]
    return jax.vmap(one_group)(group_keys, head_list).reshape(G_DEV, head_dev, TOPB)


def draw_selection(key, part):
    base_key = jax.random.fold_in(key, 7919)
    popular_key, device_key = jax.random.split(base_key)
    popular = jax.random.randint(popular_key, (), 0, N_CTX, dtype=jnp.int32)
    device_keys = jax.random.split(device_key, N_CTX * N_HEAD)
    picked = jax.vmap(lambda subkey: device_picks(subkey, popular))(device_keys)
    head_dev = HEADS // N_HEAD
    picked = picked.reshape(N_CTX, N_HEAD, G_DEV, head_dev, TOPB).transpose(0, 2, 1, 3, 4)
    return picked.reshape(NGROUP, HEADS, TOPB).astype(jnp.int32)


def block_levels(stream_key, dims, cuts, low, top_value):
    loudness, own = 1.0, jax.random.fold_in(stream_key, 6)
    for dim, shards_of in cuts:
        steps = jnp.exp(jax.random.uniform(jax.random.fold_in(own, dim), (shards_of,), jnp.float32, low / len(cuts), top_value / len(cuts)))
        loudness = loudness * jnp.repeat(steps, dims[dim] // shards_of).reshape([-1 if axis == dim else 1 for axis in range(len(dims))])
    return loudness


def gaussian(key, extent, scale, most, cuts=(), kind=jnp.bfloat16):
    factor_of = block_levels(key, extent, cuts, -0.22, 0.18) if cuts else 1.0
    entries = jax.random.normal(key, extent, jnp.float32) * scale * factor_of
    return jnp.minimum(jnp.maximum(entries, -most), most).astype(kind)


def setup_inputs(seed: int = 0) -> dict:
    arg_keys = jax.random.split(jax.random.key(seed), 10)
    queries = draw_queries(jax.random.fold_in(arg_keys[9], 71), 0)
    span_keys = draw_span_keys(jax.random.fold_in(arg_keys[9], 71), 0)
    span_values = gaussian(arg_keys[2], (SPAN, HEADS * DH), 16.0, 96.0, ((0, 16), (1, 2)))
    cache_keys = gaussian(arg_keys[3], (NCTX, HEADS * DH), 1.0, 6.0, ((0, 16), (1, 2)))
    cache_values = gaussian(arg_keys[4], (NCTX, HEADS * DH), 16.0, 96.0, ((0, 16), (1, 2)))
    land_keys = draw_land_keys(jax.random.fold_in(arg_keys[9], 71), 0)
    land_values = gaussian(arg_keys[6], (NBLK, HEADS * DH), 16.0, 96.0, ((0, 16), (1, 2)))
    out_weight = gaussian(arg_keys[7], (HEADS * DH, D), (HEADS * DH) ** -0.5, 0.09375, ((0, 2), (1, 16)))
    selection = draw_selection(jax.random.fold_in(arg_keys[9], 71), 0)
    return dict(queries=queries, span_keys=span_keys, span_values=span_values, cache_keys=cache_keys, cache_values=cache_values, land_keys=land_keys, land_values=land_values, out_weight=out_weight, selection=selection)


def reference(queries, span_keys, span_values, cache_keys, cache_values, land_keys, land_values, out_weight, selection):
    scaling = 1.0 / math.sqrt(DH)
    groups = SPAN // BLOCK
    causal = jnp.arange(BLOCK)[:, None] >= jnp.arange(BLOCK)[None, :]
    highest = lax.Precision.HIGHEST

    def rounded(weights):
        return lax.optimization_barrier(weights.astype(jnp.bfloat16)).astype(jnp.float32)

    def one_head(head_index):

        def column_cut(source):
            return lax.dynamic_slice_in_dim(source, head_index * DH, DH, 1).astype(jnp.float32)
        query_head = column_cut(queries).reshape(groups, BLOCK, DH)
        land_scores = jnp.einsum('gqd,nd->gqn', query_head, column_cut(land_keys), precision=highest) * scaling
        picked = lax.dynamic_index_in_dim(selection, head_index, 1, keepdims=False)
        key_blocks = column_cut(cache_keys).reshape(NBLK, BLOCK * DH)[picked].reshape(groups, TOPB * BLOCK, DH)
        value_blocks = column_cut(cache_values).reshape(NBLK, BLOCK * DH)[picked].reshape(groups, TOPB * BLOCK, DH)
        chosen_scores = jnp.einsum('gqd,gkd->gqk', query_head, key_blocks, precision=highest) * scaling
        local_keys = column_cut(span_keys).reshape(groups, BLOCK, DH)
        local_values = column_cut(span_values).reshape(groups, BLOCK, DH)
        local_scores = jnp.einsum('gqd,gkd->gqk', query_head, local_keys, precision=highest) * scaling
        local_scores = jnp.where(causal[None], local_scores, -jnp.inf)
        top = jnp.maximum(jnp.maximum(lax.optimization_barrier(jnp.max(land_scores, axis=2)), lax.optimization_barrier(jnp.max(chosen_scores, axis=2))), lax.optimization_barrier(jnp.max(local_scores, axis=2)))
        land_weights = jnp.exp(land_scores - top[:, :, None])
        chosen_weights = jnp.exp(chosen_scores - top[:, :, None])
        local_weights = jnp.exp(local_scores - top[:, :, None])
        summed_weights = lax.optimization_barrier(jnp.sum(land_weights, axis=2)) + lax.optimization_barrier(jnp.sum(chosen_weights, axis=2)) + lax.optimization_barrier(jnp.sum(local_weights, axis=2))
        numerator = jnp.einsum('gqn,nd->gqd', rounded(land_weights), column_cut(land_values), precision=highest)
        numerator = numerator + jnp.einsum('gqk,gkd->gqd', rounded(chosen_weights), value_blocks, precision=highest)
        numerator = numerator + jnp.einsum('gqk,gkd->gqd', rounded(local_weights), local_values, precision=highest)
        return (numerator / summed_weights[:, :, None]).reshape(SPAN, DH).astype(jnp.bfloat16)
    heads_out = lax.map(one_head, jnp.arange(HEADS, dtype=jnp.int32))
    attended = jnp.transpose(heads_out, (1, 0, 2)).reshape(SPAN, HEADS * DH)
    head_width = HEADS // N_HEAD * DH
    summed = jnp.zeros((SPAN, D), jnp.float32)
    for head_shard in range(N_HEAD):
        rows_in = attended[:, head_shard * head_width:(head_shard + 1) * head_width].astype(jnp.float32)
        rows_weight = out_weight[head_shard * head_width:(head_shard + 1) * head_width].astype(jnp.float32)
        partial_value = jnp.dot(rows_in, rows_weight, precision=highest)
        summed = summed + rounded(partial_value)
    return summed.astype(jnp.bfloat16)
```

```python
import functools
import math

import jax
import jax.numpy as jnp
from jax import lax
from jax.experimental import pallas as pl
from jax.experimental.pallas import tpu as pltpu
from jax.sharding import PartitionSpec as P

BLOCK = 64
ANY = pl.BlockSpec(memory_space=pl.ANY)
VMEM = pl.BlockSpec(memory_space=pltpu.VMEM)
SMEM = pl.BlockSpec(memory_space=pltpu.SMEM)
LIMIT = 60 * 1024 * 1024


def split_ctx(devices, head_devices):
    fast = 1
    while (
        (2 * fast) ** 2 <= devices
        and devices % (2 * fast) == 0
        and (devices // (2 * fast)) % head_devices == 0
    ):
        fast *= 2
    return devices // fast, fast


def exchange_tables(selection, blocks_dev, devices):
    groups, heads, picks = selection.shape
    count = groups * heads * picks
    most = (heads * 2 * picks + devices - 1) // devices
    head = lax.broadcasted_iota(jnp.int32, selection.shape, 1)
    owner = (selection // blocks_dev).reshape(count)
    code = ((selection % blocks_dev) * heads + head).reshape(count)
    pair = (selection * heads + head).reshape(count)
    order = jnp.arange(count)
    earlier = order[None, :] < order[:, None]
    same_pair = pair[:, None] == pair[None, :]
    same_owner = owner[:, None] == owner[None, :]
    first = jnp.logical_not(jnp.any(same_pair & earlier, axis=1))
    rank = jnp.sum((same_owner & earlier & first[None, :]).astype(jnp.int32), axis=1)
    slot = jnp.sum(jnp.where(same_pair & first[None, :], rank[None, :], 0), axis=1)
    cell = owner * most + slot
    cells = jnp.arange(devices * most)
    asked = jnp.sum(
        jnp.where((cells[:, None] == cell[None, :]) & first[None, :], code[None, :], 0), axis=1
    )
    return cell, asked.reshape(devices, most)


def gather_kernel(heads, asked_ref, source_ref, out_ref, sem):
    size = out_ref.shape[2]

    def start(cell, carry):
        code = asked_ref[cell]
        row = pl.multiple_of(lax.div(code, heads) * BLOCK, BLOCK)
        column = pl.multiple_of(lax.rem(code, heads) * size, size)
        pltpu.make_async_copy(
            source_ref.at[pl.ds(row, BLOCK), pl.ds(column, size)], out_ref.at[cell], sem
        ).start()
        return carry

    lax.fori_loop(0, out_ref.shape[0], start, 0)
    pltpu.make_async_copy(out_ref, out_ref, sem).wait()


def gather_blocks(asked, source, heads):
    cells = asked.shape[0]
    size = source.shape[1] // heads
    return pl.pallas_call(
        functools.partial(gather_kernel, heads),
        out_shape=jax.ShapeDtypeStruct((cells, BLOCK, size), source.dtype),
        in_specs=[SMEM, ANY],
        out_specs=VMEM,
        scratch_shapes=[pltpu.SemaphoreType.DMA],
        cost_estimate=pl.CostEstimate(
            flops=cells * BLOCK * size * 64,
            bytes_accessed=4 * cells * BLOCK * size,
            transcendentals=0,
        ),
        name="gather_blocks",
    )(asked, source)


def nt_dot(a, b):
    return lax.dot_general(a, b, (((1,), (1,)), ((), ())), preferred_element_type=jnp.float32)


def score_kernel(
    groups, heads, picks, step_heads, cell_ref, q_ref, land_ref, lk_ref, lv_ref, fk_ref,
    weight_ref, acc_ref,
):
    size = q_ref.shape[1] // step_heads
    scaling = 1.0 / math.sqrt(size)
    first_head = pl.program_id(0) * step_heads
    row = lax.broadcasted_iota(jnp.int32, (BLOCK, BLOCK), 0)
    column = lax.broadcasted_iota(jnp.int32, (BLOCK, BLOCK), 1)
    causal = row >= column
    pieces, _, land_rows, _ = land_ref.shape
    chosen = picks * BLOCK
    for hh in range(step_heads):
        cols = slice(hh * size, (hh + 1) * size)
        land_k = land_ref[:, 0, :, cols].reshape(pieces * land_rows, size)
        land_v = land_ref[:, 1, :, cols].reshape(pieces * land_rows, size)
        for g in range(groups):
            rows = slice(g * BLOCK, (g + 1) * BLOCK)
            q = q_ref[rows, cols]
            base = (g * heads + first_head + hh) * picks
            keys = jnp.concatenate([fk_ref[cell_ref[base + p]] for p in range(picks)], axis=0)
            s_land = nt_dot(q, land_k) * scaling
            s_chosen = nt_dot(q, keys) * scaling
            s_local = jnp.where(causal, nt_dot(q, lk_ref[rows, cols]) * scaling, -jnp.inf)
            top = jnp.maximum(
                jnp.maximum(
                    jnp.max(s_land, axis=1, keepdims=True),
                    jnp.max(s_chosen, axis=1, keepdims=True),
                ),
                jnp.max(s_local, axis=1, keepdims=True),
            )
            w_land = jnp.exp(s_land - top)
            w_chosen = jnp.exp(s_chosen - top)
            w_local = jnp.exp(s_local - top)
            total = (
                jnp.sum(w_land, axis=1, keepdims=True)
                + jnp.sum(w_chosen, axis=1, keepdims=True)
                + jnp.sum(w_local, axis=1, keepdims=True)
            )
            inverse = 1.0 / total
            part = jnp.dot(
                w_land.astype(jnp.bfloat16), land_v, preferred_element_type=jnp.float32
            ) + jnp.dot(
                w_local.astype(jnp.bfloat16), lv_ref[rows, cols], preferred_element_type=jnp.float32
            )
            acc_ref[rows, cols] = part * inverse
            weight_ref[rows, hh * chosen : (hh + 1) * chosen] = (w_chosen * inverse).astype(
                jnp.bfloat16
            )


def value_kernel(groups, heads, picks, step_heads, cell_ref, weight_ref, acc_ref, fv_ref, out_ref):
    size = acc_ref.shape[1] // step_heads
    first_head = pl.program_id(0) * step_heads
    chosen = picks * BLOCK
    for hh in range(step_heads):
        cols = slice(hh * size, (hh + 1) * size)
        for g in range(groups):
            rows = slice(g * BLOCK, (g + 1) * BLOCK)
            base = (g * heads + first_head + hh) * picks
            values = jnp.concatenate([fv_ref[cell_ref[base + p]] for p in range(picks)], axis=0)
            out_ref[rows, cols] = (
                acc_ref[rows, cols]
                + jnp.dot(
                    weight_ref[rows, hh * chosen : (hh + 1) * chosen],
                    values,
                    preferred_element_type=jnp.float32,
                )
            ).astype(out_ref.dtype)


def attention_scores(cell, queries, land, span_keys, span_values, fetched_keys, dims):
    groups, heads, picks = dims
    rows, width = queries.shape
    size = width // heads
    step = math.gcd(heads, 4)
    wide = step * size
    chosen = picks * BLOCK
    by_head = lambda i, c: (0, i)
    keys = land.shape[0] * land.shape[2] + chosen + BLOCK
    return pl.pallas_call(
        functools.partial(score_kernel, groups, heads, picks, step),
        grid_spec=pltpu.PrefetchScalarGridSpec(
            num_scalar_prefetch=1,
            grid=(heads // step,),
            in_specs=[
                pl.BlockSpec((rows, wide), by_head),
                pl.BlockSpec(land.shape[:3] + (wide,), lambda i, c: (0, 0, 0, i)),
                pl.BlockSpec((rows, wide), by_head),
                pl.BlockSpec((rows, wide), by_head),
                pl.BlockSpec(fetched_keys.shape, lambda i, c: (0, 0, 0)),
            ],
            out_specs=[
                pl.BlockSpec((rows, step * chosen), by_head),
                pl.BlockSpec((rows, wide), by_head),
            ],
        ),
        out_shape=[
            jax.ShapeDtypeStruct((rows, heads * chosen), jnp.bfloat16),
            jax.ShapeDtypeStruct((rows, width), jnp.float32),
        ],
        compiler_params=pltpu.CompilerParams(vmem_limit_bytes=LIMIT),
        cost_estimate=pl.CostEstimate(
            flops=16 * rows * keys * width,
            bytes_accessed=16 * rows * width,
            transcendentals=rows * keys * heads,
        ),
        name="attention_scores",
    )(cell, queries, land, span_keys, span_values, fetched_keys)


def attention_values(cell, weights, part, fetched_values, dims):
    groups, heads, picks = dims
    rows, width = part.shape
    size = width // heads
    step = math.gcd(heads, 4)
    wide = step * size
    chosen = picks * BLOCK
    by_head = lambda i, c: (0, i)
    return pl.pallas_call(
        functools.partial(value_kernel, groups, heads, picks, step),
        grid_spec=pltpu.PrefetchScalarGridSpec(
            num_scalar_prefetch=1,
            grid=(heads // step,),
            in_specs=[
                pl.BlockSpec((rows, step * chosen), by_head),
                pl.BlockSpec((rows, wide), by_head),
                pl.BlockSpec(fetched_values.shape, lambda i, c: (0, 0, 0)),
            ],
            out_specs=pl.BlockSpec((rows, wide), by_head),
        ),
        out_shape=jax.ShapeDtypeStruct((rows, width), jnp.bfloat16),
        compiler_params=pltpu.CompilerParams(vmem_limit_bytes=LIMIT),
        cost_estimate=pl.CostEstimate(
            flops=4 * rows * chosen * width,
            bytes_accessed=12 * rows * width,
            transcendentals=0,
        ),
        name="attention_values",
    )(cell, weights, part, fetched_values)


def project_kernel(slow_count, head_devices, pieces, place_ref, *refs):
    a_refs, b_refs = refs[:pieces], refs[pieces : pieces + 2 * slow_count - 1]
    mine_ref, send_ref, b_buf, sem = refs[pieces + 2 * slow_count - 1 :]
    slow, head = place_ref[0], place_ref[1]
    share = slow_count // head_devices
    width = b_buf.shape[2]
    for slot in range(slow_count):
        target = lax.rem(head + slot // share, head_devices) * share + slot % share
        for index in range(2 * slow_count - 1):

            @pl.when(target - slow == index - (slow_count - 1))
            def _():
                pltpu.make_async_copy(b_refs[index], b_buf.at[slot], sem.at[slot]).start()

    for slot in range(slow_count):
        pltpu.make_async_copy(b_refs[0], b_buf.at[slot], sem.at[slot]).wait()
        row = 0
        for a_ref in a_refs:
            rows = slice(row, row + a_ref.shape[0])
            row += a_ref.shape[0]
            product = jnp.dot(a_ref[...], b_buf[slot], preferred_element_type=jnp.float32)
            if slot < share:
                mine_ref[rows, slot * width : (slot + 1) * width] = product
            else:
                other = slot - share
                send_ref[
                    other // share, rows, (other % share) * width : (other % share + 1) * width
                ] = product.astype(send_ref.dtype)


def project(place, a_pieces, b_blocks, slow_count, head_devices):
    rows = sum(a.shape[0] for a in a_pieces)
    depth, width = b_blocks[0].shape
    share = slow_count // head_devices
    return pl.pallas_call(
        functools.partial(project_kernel, slow_count, head_devices, len(a_pieces)),
        out_shape=[
            jax.ShapeDtypeStruct((rows, share * width), jnp.float32),
            jax.ShapeDtypeStruct((head_devices - 1, rows, share * width), jnp.bfloat16),
        ],
        in_specs=[SMEM] + [VMEM] * len(a_pieces) + [ANY] * len(b_blocks),
        out_specs=[VMEM, VMEM],
        scratch_shapes=[
            pltpu.VMEM((slow_count, depth, width), jnp.bfloat16),
            pltpu.SemaphoreType.DMA((slow_count,)),
        ],
        compiler_params=pltpu.CompilerParams(vmem_limit_bytes=LIMIT),
        cost_estimate=pl.CostEstimate(
            flops=2 * rows * depth * width * slow_count,
            bytes_accessed=2 * depth * width * slow_count,
            transcendentals=0,
        ),
        name="project",
    )(place, *a_pieces, *b_blocks)


def assemble_kernel(fast_count, share, others, place_ref, mine_ref, *refs):
    received, tiles, out_ref = refs[:others], refs[others:-1], refs[-1]
    width = mine_ref.shape[1] // share
    for fast in range(fast_count):

        @pl.when(place_ref[2] == fast)
        def _():
            for mask in range(fast_count):
                for block in range(share):
                    cols = slice(block * width, (block + 1) * width)
                    if mask == 0:
                        total = mine_ref[:, cols]
                        for other in received:
                            total = total + other[:, cols].astype(jnp.float32)
                        tile = total.astype(out_ref.dtype)
                    else:
                        tile = tiles[mask - 1][:, cols]
                    start = (block * fast_count + (fast ^ mask)) * width
                    out_ref[:, start : start + width] = tile


def assemble(place, mine, received, tiles, share):
    fast_count = len(tiles) + 1
    rows, wide = mine.shape
    return pl.pallas_call(
        functools.partial(assemble_kernel, fast_count, share, len(received)),
        out_shape=jax.ShapeDtypeStruct((rows, wide * fast_count), jnp.bfloat16),
        in_specs=[SMEM] + [VMEM] * (1 + len(received) + len(tiles)),
        out_specs=VMEM,
        name="assemble",
    )(place, mine, *received, *tiles)


def local(
    queries,
    span_keys,
    span_values,
    cache_keys,
    cache_values,
    land_keys,
    land_values,
    out_weight,
    selection,
):
    rows, width = queries.shape
    groups, heads, picks = selection.shape
    size = width // heads
    devices = lax.axis_size("ctx")
    head_devices = lax.axis_size("head")
    slow_count, fast_count = split_ctx(devices, head_devices)
    share = slow_count // head_devices
    bits = [1 << k for k in range(fast_count.bit_length() - 1)]
    index = lax.axis_index("ctx")
    place = jnp.stack([index // fast_count, lax.axis_index("head"), index % fast_count])
    place = place.astype(jnp.int32)

    def across(value, mask):
        return lax.ppermute(value, "ctx", [(i, i ^ mask) for i in range(devices)])

    def along(value, shift, low=0, high=None):
        high = slow_count if high is None else high
        pairs = [
            (s * fast_count + f, (s + shift) * fast_count + f)
            for s in range(low, high)
            for f in range(fast_count)
            if 0 <= s + shift < slow_count
        ]
        return lax.ppermute(value, "ctx", pairs)

    blocks_dev = cache_keys.shape[0] // BLOCK
    cell, asked = exchange_tables(selection, blocks_dev, devices)
    asked_for = lax.all_to_all(asked, "ctx", split_axis=0, concat_axis=0, tiled=True)
    asked_for = asked_for.reshape(-1)

    below, above = [out_weight], [out_weight]
    if slow_count > 1:
        below.append(along(out_weight, 1))
        above.append(along(out_weight, -1))
    land = jnp.stack([land_keys, land_values])[None]
    land_parts = [land]
    for shift in range(1, slow_count):
        pairs = [
            (s * fast_count + f, (s + shift) % slow_count * fast_count + f)
            for s in range(slow_count)
            for f in range(fast_count)
        ]
        land_parts.append(lax.ppermute(land, "ctx", pairs))
    land = jnp.concatenate(land_parts, axis=0)
    for bit in bits:
        land = jnp.concatenate([land, across(land, bit)], axis=0)

    def fetch(source):
        sent = gather_blocks(asked_for, source, heads).reshape(devices, -1, BLOCK, size)
        got = lax.all_to_all(sent, "ctx", split_axis=0, concat_axis=0, tiled=True)
        return got.reshape(-1, BLOCK, size)

    fetched_keys = fetch(cache_keys)
    fetched_values = fetch(cache_values)

    dims = (groups, heads, picks)
    weights, part = attention_scores(
        cell, queries, land, span_keys, span_values, fetched_keys, dims
    )
    attended = attention_values(cell, weights, part, fetched_values, dims)

    for hop in range(2, slow_count):
        low, high = below[-1], above[-1]
        if hop == 2:
            low, high, _ = lax.optimization_barrier((low, high, fetched_values))
        below.append(along(low, 1, hop - 1, slow_count))
        above.append(along(high, -1, 0, slow_count - hop + 1))
    b_blocks = below[:0:-1] + [out_weight] + above[1:]

    pieces = {0: [attended]}
    for mask in sorted(range(1, fast_count), key=lambda m: (m.bit_count(), m)):
        own = [b for b in bits if b & mask]
        if len(own) == 1:
            pieces[mask] = [across(attended, mask)]
            continue
        edges = [rows * k // len(own) for k in range(len(own) + 1)]
        pieces[mask] = []
        for k, bit in enumerate(own):
            whole = pieces[mask ^ bit]
            whole = whole[0] if len(whole) == 1 else jnp.concatenate(whole, axis=0)
            pieces[mask].append(across(whole[edges[k] : edges[k + 1]], bit))

    tiles = {}
    for mask in [*range(1, fast_count), 0]:
        mine, send = project(place, pieces[mask], b_blocks, slow_count, head_devices)
        received = [
            lax.ppermute(
                send[r - 1], "head", [(h, (h + r) % head_devices) for h in range(head_devices)]
            )
            for r in range(1, head_devices)
        ]
        if mask == 0:
            break
        total = mine
        for other in received:
            total = total + other.astype(jnp.float32)
        tiles[mask] = across(total.astype(jnp.bfloat16), mask)
    return assemble(place, mine, received, [tiles[m] for m in range(1, fast_count)], share)


def solution(mesh):
    placed = (
        P("ctx", "head"),
        P("ctx", "head"),
        P("ctx", "head"),
        P("ctx", "head"),
        P("ctx", "head"),
        P("ctx", "head"),
        P("ctx", "head"),
        P("head", "ctx"),
        P("ctx", "head", None),
    )
    return jax.shard_map(
        local, mesh=mesh, in_specs=placed, out_specs=P("ctx", "head"), check_vma=False
    )
```

```python
import functools
import math

import jax
import jax.numpy as jnp
from jax import lax
from jax.experimental import pallas as pl
from jax.experimental.pallas import tpu as pltpu
from jax.sharding import PartitionSpec as P


BLOCK = 64
HBM = pl.BlockSpec(memory_space=pltpu.HBM)
VMEM = pl.BlockSpec(memory_space=pltpu.VMEM)
SMEM = pl.BlockSpec(memory_space=pltpu.SMEM)
LIMIT = 24 * 1024 * 1024


def split_ctx(devices, head_devices):
    fast = 1
    while (
        (2 * fast) ** 2 <= devices
        and devices % (2 * fast) == 0
        and (devices // (2 * fast)) % head_devices == 0
    ):
        fast *= 2
    return devices // fast, fast


def exchange_tables(selection, blocks_dev, devices):
    groups, heads, picks = selection.shape
    count = groups * heads * picks
    most = (heads * 2 * picks + devices - 1) // devices
    head = lax.broadcasted_iota(jnp.int32, selection.shape, 1)
    owner = (selection // blocks_dev).reshape(count)
    code = ((selection % blocks_dev) * heads + head).reshape(count)
    pair = (selection * heads + head).reshape(count)
    order = jnp.arange(count)
    earlier = order[None, :] < order[:, None]
    same_pair = pair[:, None] == pair[None, :]
    same_owner = owner[:, None] == owner[None, :]
    first = jnp.logical_not(jnp.any(same_pair & earlier, axis=1))
    rank = jnp.sum((same_owner & earlier & first[None, :]).astype(jnp.int32), axis=1)
    slot = jnp.sum(jnp.where(same_pair & first[None, :], rank[None, :], 0), axis=1)
    cell = owner * most + slot
    cells = jnp.arange(devices * most)
    asked = jnp.sum(
        jnp.where((cells[:, None] == cell[None, :]) & first[None, :], code[None, :], 0), axis=1
    )
    return cell, asked.reshape(devices, most)


def gather_kernel(heads, asked_ref, source_ref, out_ref, sem):
    size = out_ref.shape[2]

    def start(cell, carry):
        code = asked_ref[cell]
        row = pl.multiple_of(lax.div(code, heads) * BLOCK, BLOCK)
        column = pl.multiple_of(lax.rem(code, heads) * size, size)
        pltpu.make_async_copy(
            source_ref.at[pl.ds(row, BLOCK), pl.ds(column, size)], out_ref.at[cell], sem
        ).start()
        return carry

    lax.fori_loop(0, out_ref.shape[0], start, 0)
    pltpu.make_async_copy(out_ref, out_ref, sem).wait()


def gather_blocks(asked, source, heads):
    cells = asked.shape[0]
    size = source.shape[1] // heads
    return pl.pallas_call(
        functools.partial(gather_kernel, heads),
        out_shape=jax.ShapeDtypeStruct((cells, BLOCK, size), source.dtype),
        in_specs=[SMEM, HBM],
        out_specs=VMEM,
        scratch_shapes=[pltpu.SemaphoreType.DMA],
        cost_estimate=pl.CostEstimate(
            flops=cells * BLOCK * size * 64,
            bytes_accessed=4 * cells * BLOCK * size,
            transcendentals=0,
        ),
        name="gather_blocks",
    )(asked, source)


def nt_dot(a, b):
    return lax.dot_general(a, b, (((1,), (1,)), ((), ())), preferred_element_type=jnp.float32)


def score_kernel(
    groups, heads, picks, step_heads, cell_ref, q_ref, land_ref, lk_ref, lv_ref, fk_ref,
    weight_ref, acc_ref,
):
    size = q_ref.shape[1] // step_heads
    scaling = 1.0 / math.sqrt(size)
    first_head = pl.program_id(0) * step_heads
    row = lax.broadcasted_iota(jnp.int32, (BLOCK, BLOCK), 0)
    column = lax.broadcasted_iota(jnp.int32, (BLOCK, BLOCK), 1)
    causal = row >= column
    pieces, _, land_rows, _ = land_ref.shape
    chosen = picks * BLOCK
    for hh in range(step_heads):
        cols = slice(hh * size, (hh + 1) * size)
        land_k = land_ref[:, 0, :, cols].reshape(pieces * land_rows, size)
        land_v = land_ref[:, 1, :, cols].reshape(pieces * land_rows, size)
        for g in range(groups):
            rows = slice(g * BLOCK, (g + 1) * BLOCK)
            q = q_ref[rows, cols]
            base = (g * heads + first_head + hh) * picks
            keys = jnp.concatenate([fk_ref[cell_ref[base + p]] for p in range(picks)], axis=0)
            s_land = nt_dot(q, land_k) * scaling
            s_chosen = nt_dot(q, keys) * scaling
            s_local = jnp.where(causal, nt_dot(q, lk_ref[rows, cols]) * scaling, -jnp.inf)
            top = jnp.maximum(
                jnp.maximum(
                    jnp.max(s_land, axis=1, keepdims=True),
                    jnp.max(s_chosen, axis=1, keepdims=True),
                ),
                jnp.max(s_local, axis=1, keepdims=True),
            )
            w_land = jnp.exp(s_land - top)
            w_chosen = jnp.exp(s_chosen - top)
            w_local = jnp.exp(s_local - top)
            total = (
                jnp.sum(w_land, axis=1, keepdims=True)
                + jnp.sum(w_chosen, axis=1, keepdims=True)
                + jnp.sum(w_local, axis=1, keepdims=True)
            )
            inverse = 1.0 / total
            part = jnp.dot(
                w_land.astype(jnp.bfloat16), land_v, preferred_element_type=jnp.float32
            ) + jnp.dot(
                w_local.astype(jnp.bfloat16), lv_ref[rows, cols], preferred_element_type=jnp.float32
            )
            acc_ref[rows, cols] = part * inverse
            weight_ref[rows, hh * chosen : (hh + 1) * chosen] = (w_chosen * inverse).astype(
                jnp.bfloat16
            )


def value_kernel(groups, heads, picks, step_heads, cell_ref, weight_ref, acc_ref, fv_ref, *outs):
    size = acc_ref.shape[1] // step_heads
    first_head = pl.program_id(0) * step_heads
    chosen = picks * BLOCK
    for hh in range(step_heads):
        cols = slice(hh * size, (hh + 1) * size)
        for g in range(groups):
            rows = slice(g * BLOCK, (g + 1) * BLOCK)
            chunk, inner = divmod(g, groups // len(outs))
            base = (g * heads + first_head + hh) * picks
            values = jnp.concatenate([fv_ref[cell_ref[base + p]] for p in range(picks)], axis=0)
            outs[chunk][inner * BLOCK : (inner + 1) * BLOCK, cols] = (
                acc_ref[rows, cols]
                + jnp.dot(
                    weight_ref[rows, hh * chosen : (hh + 1) * chosen],
                    values,
                    preferred_element_type=jnp.float32,
                )
            ).astype(jnp.bfloat16)


def attention_scores(cell, queries, land, span_keys, span_values, fetched_keys, dims):
    groups, heads, picks = dims
    rows, width = queries.shape
    size = width // heads
    step = math.gcd(heads, 4)
    wide = step * size
    chosen = picks * BLOCK
    by_head = lambda i, c: (0, i)
    keys = land.shape[0] * land.shape[2] + chosen + BLOCK
    return pl.pallas_call(
        functools.partial(score_kernel, groups, heads, picks, step),
        grid_spec=pltpu.PrefetchScalarGridSpec(
            num_scalar_prefetch=1,
            grid=(heads // step,),
            in_specs=[
                pl.BlockSpec((rows, wide), by_head),
                pl.BlockSpec(land.shape[:3] + (wide,), lambda i, c: (0, 0, 0, i)),
                pl.BlockSpec((rows, wide), by_head),
                pl.BlockSpec((rows, wide), by_head),
                pl.BlockSpec(fetched_keys.shape, lambda i, c: (0, 0, 0)),
            ],
            out_specs=[
                pl.BlockSpec((rows, step * chosen), by_head),
                pl.BlockSpec((rows, wide), by_head),
            ],
        ),
        out_shape=[
            jax.ShapeDtypeStruct((rows, heads * chosen), jnp.bfloat16),
            jax.ShapeDtypeStruct((rows, width), jnp.float32),
        ],
        compiler_params=pltpu.CompilerParams(vmem_limit_bytes=LIMIT),
        cost_estimate=pl.CostEstimate(
            flops=16 * rows * keys * width,
            bytes_accessed=16 * rows * width,
            transcendentals=rows * keys * heads,
        ),
        name="attention_scores",
    )(cell, queries, land, span_keys, span_values, fetched_keys)


def attention_values(cell, weights, part, fetched_values, dims):
    groups, heads, picks = dims
    rows, width = part.shape
    size = width // heads
    step = math.gcd(heads, 4)
    wide = step * size
    chosen = picks * BLOCK
    chunks = math.gcd(groups, 2)
    by_head = lambda i, c: (0, i)
    return pl.pallas_call(
        functools.partial(value_kernel, groups, heads, picks, step),
        grid_spec=pltpu.PrefetchScalarGridSpec(
            num_scalar_prefetch=1,
            grid=(heads // step,),
            in_specs=[
                pl.BlockSpec((rows, step * chosen), by_head),
                pl.BlockSpec((rows, wide), by_head),
                pl.BlockSpec(fetched_values.shape, lambda i, c: (0, 0, 0)),
            ],
            out_specs=[pl.BlockSpec((rows // chunks, wide), by_head)] * chunks,
        ),
        out_shape=[jax.ShapeDtypeStruct((rows // chunks, width), jnp.bfloat16)] * chunks,
        compiler_params=pltpu.CompilerParams(vmem_limit_bytes=LIMIT),
        cost_estimate=pl.CostEstimate(
            flops=4 * rows * chosen * width,
            bytes_accessed=12 * rows * width,
            transcendentals=0,
        ),
        name="attention_values",
    )(cell, weights, part, fetched_values)


def pick_kernel(slow_count, head_devices, table, place_ref, *refs):
    b_refs, out_ref, sem = refs[:-2], refs[-2], refs[-1]
    slow, head = place_ref[0], place_ref[1]
    share = slow_count // head_devices
    for slot in range(slow_count):
        target = lax.rem(head + slot // share, head_devices) * share + slot % share
        for step, low, high, members in table:

            @pl.when((target - slow == step) & (slow >= low) & (slow <= high))
            def _():
                row = 0
                for member in members:
                    ref = b_refs[member]
                    rows = pl.ds(row, ref.shape[0])
                    row += ref.shape[0]
                    pltpu.make_async_copy(ref, out_ref.at[slot, rows], sem.at[slot]).start()

    for slot in range(slow_count):
        pltpu.make_async_copy(out_ref.at[slot], out_ref.at[slot], sem.at[slot]).wait()


def pick(place, blocks, slow_count, head_devices):
    arrays, table = [], []
    for step, low, high, chunks in blocks:
        table.append((step, low, high, range(len(arrays), len(arrays) + len(chunks))))
        arrays += chunks
    depth, width = sum(c.shape[0] for c in blocks[0][3]), arrays[0].shape[1]
    return pl.pallas_call(
        functools.partial(pick_kernel, slow_count, head_devices, table),
        out_shape=jax.ShapeDtypeStruct((slow_count, depth, width), jnp.bfloat16),
        in_specs=[SMEM] + [HBM] * len(arrays),
        out_specs=VMEM,
        scratch_shapes=[pltpu.SemaphoreType.DMA((slow_count,))],
        compiler_params=pltpu.CompilerParams(vmem_limit_bytes=60 * 1024 * 1024),
        cost_estimate=pl.CostEstimate(
            flops=64 * depth * width * slow_count,
            bytes_accessed=4 * depth * width * slow_count,
            transcendentals=0,
        ),
        name="pick",
    )(place, *arrays)


def project_kernel(share, a_count, *refs):
    a_refs, (b_ref, mine_ref, send_ref) = refs[:a_count], refs[a_count:]
    slots, _, width = b_ref.shape
    for slot in range(slots):
        row = 0
        for a_ref in a_refs:
            rows = slice(row, row + a_ref.shape[0])
            row += a_ref.shape[0]
            product = jnp.dot(a_ref[...], b_ref[slot], preferred_element_type=jnp.float32)
            cols = slice(slot % share * width, (slot % share + 1) * width)
            if slot < share:
                mine_ref[rows, cols] = product
            else:
                send_ref[slot // share - 1, rows, cols] = product.astype(send_ref.dtype)


def project(a_pieces, b_all, share):
    rows = sum(a.shape[0] for a in a_pieces)
    slots, depth, width = b_all.shape
    return pl.pallas_call(
        functools.partial(project_kernel, share, len(a_pieces)),
        out_shape=[
            jax.ShapeDtypeStruct((rows, share * width), jnp.float32),
            jax.ShapeDtypeStruct((slots // share - 1, rows, share * width), jnp.bfloat16),
        ],
        in_specs=[VMEM] * (len(a_pieces) + 1),
        out_specs=[VMEM, VMEM],
        compiler_params=pltpu.CompilerParams(vmem_limit_bytes=LIMIT // 2),
        cost_estimate=pl.CostEstimate(
            flops=2 * rows * depth * width * slots,
            bytes_accessed=2 * depth * width * slots,
            transcendentals=0,
        ),
        name="project",
    )(*a_pieces, b_all)


def assemble_kernel(fast_count, share, others, place_ref, mine_ref, *refs):
    received, tiles, out_ref = refs[:others], refs[others:-1], refs[-1]
    width = mine_ref.shape[1] // share
    for fast in range(fast_count):

        @pl.when(place_ref[2] == fast)
        def _():
            for mask in range(fast_count):
                for block in range(share):
                    cols = slice(block * width, (block + 1) * width)
                    if mask == 0:
                        total = mine_ref[:, cols]
                        for other in received:
                            total = total + other[:, cols].astype(jnp.float32)
                        tile = total.astype(out_ref.dtype)
                    else:
                        tile = tiles[mask - 1][:, cols]
                    start = (block * fast_count + (fast ^ mask)) * width
                    out_ref[:, start : start + width] = tile


def assemble(place, mine, received, tiles, share):
    fast_count = len(tiles) + 1
    rows, wide = mine.shape
    return pl.pallas_call(
        functools.partial(assemble_kernel, fast_count, share, len(received)),
        out_shape=jax.ShapeDtypeStruct((rows, wide * fast_count), jnp.bfloat16),
        in_specs=[SMEM] + [VMEM] * (1 + len(received) + len(tiles)),
        out_specs=VMEM,
        name="assemble",
    )(place, mine, *received, *tiles)


def local(
    queries,
    span_keys,
    span_values,
    cache_keys,
    cache_values,
    land_keys,
    land_values,
    out_weight,
    selection,
):
    _, width = queries.shape
    groups, heads, picks = selection.shape
    size = width // heads
    devices = lax.axis_size("ctx")
    head_devices = lax.axis_size("head")
    slow_count, fast_count = split_ctx(devices, head_devices)
    share = slow_count // head_devices
    bits = [1 << k for k in range(fast_count.bit_length() - 1)]
    index = lax.axis_index("ctx")
    place = jnp.stack([index // fast_count, lax.axis_index("head"), index % fast_count])
    place = place.astype(jnp.int32)

    def across(value, mask):
        return lax.ppermute(value, "ctx", [(i, i ^ mask) for i in range(devices)])

    def along(value, shift, low=0, high=None):
        high = slow_count if high is None else high
        pairs = [
            (s * fast_count + f, (s + shift) * fast_count + f)
            for s in range(low, high)
            for f in range(fast_count)
            if 0 <= s + shift < slow_count
        ]
        return lax.ppermute(value, "ctx", pairs)

    blocks_dev = cache_keys.shape[0] // BLOCK
    cell, asked = exchange_tables(selection, blocks_dev, devices)
    asked_for = lax.all_to_all(asked, "ctx", split_axis=0, concat_axis=0, tiled=True)
    asked_for = asked_for.reshape(-1)

    last = slow_count - 1
    blocks = [(0, 0, last, [out_weight])]
    low_parts = high_parts = None
    if slow_count > 1:
        low, high = along(out_weight, 1), along(out_weight, -1)
        blocks += [(-1, 1, last, [low]), (1, 0, last - 1, [high])]
    if slow_count > 2:
        blocks.append((-2, last, last, [along(low, 1, last - 1, last)]))
        blocks.append((2, 0, 0, [along(high, -1, 1, 2)]))
        cut = low.shape[0] // 2
        low_parts, high_parts = [low[:cut], low[cut:]], [high[:cut], high[cut:]]
    land = jnp.stack([land_keys, land_values])[None]
    land_parts = [land]
    for shift in range(1, slow_count):
        pairs = [
            (s * fast_count + f, (s + shift) % slow_count * fast_count + f)
            for s in range(slow_count)
            for f in range(fast_count)
        ]
        land_parts.append(lax.ppermute(land, "ctx", pairs))
    land = jnp.concatenate(land_parts, axis=0)
    for bit in bits:
        land = jnp.concatenate([land, across(land, bit)], axis=0)

    def fetch(source):
        sent = gather_blocks(asked_for, source, heads).reshape(devices, -1, BLOCK, size)
        got = lax.all_to_all(sent, "ctx", split_axis=0, concat_axis=0, tiled=True)
        return got.reshape(-1, BLOCK, size)

    fetched_keys = fetch(cache_keys)
    fetched_values = fetch(cache_values)

    dims = (groups, heads, picks)
    weights, part = attention_scores(
        cell, queries, land, span_keys, span_values, fetched_keys, dims
    )
    attended = attention_values(cell, weights, part, fetched_values, dims)

    if slow_count > 3:
        low_parts, high_parts, _ = lax.optimization_barrier(
            (low_parts, high_parts, fetched_values)
        )
    for hop in range(2, slow_count):
        top = last - 1 if hop == 2 else last
        if hop > top:
            break
        for j in range(2):
            low_parts[j] = along(low_parts[j], 1, hop - 1, top)
            high_parts[j] = along(high_parts[j], -1, last - top + 1, last - hop + 2)
        low_parts, high_parts = list(low_parts), list(high_parts)
        blocks.append((-hop, hop, top, list(low_parts)))
        blocks.append((hop, last - top, last - hop, list(high_parts)))

    chunks = len(attended)
    pieces = {0: attended}
    masks = sorted(range(1, fast_count), key=lambda m: (m.bit_count(), m))
    for mask in masks:
        own = [b for b in bits if b & mask]
        pieces[mask] = [None] * chunks
        for j in reversed(range(chunks)) if mask == 1 else range(chunks):
            bit = own[j % len(own)]
            pieces[mask][j] = across(pieces[mask ^ bit][j], bit)

    b_all = pick(place, blocks, slow_count, head_devices)
    tiles = {}
    for mask in [*reversed(masks), 0]:
        mine, send = project(pieces[mask], b_all, share)
        received = [
            lax.ppermute(
                send[r - 1], "head", [(h, (h + r) % head_devices) for h in range(head_devices)]
            )
            for r in range(1, head_devices)
        ]
        if mask == 0:
            break
        total = mine
        for other in received:
            total = total + other.astype(jnp.float32)
        tiles[mask] = across(total.astype(jnp.bfloat16), mask)
    return assemble(place, mine, received, [tiles[m] for m in range(1, fast_count)], share)


def solution(mesh):
    placed = (
        P("ctx", "head"),
        P("ctx", "head"),
        P("ctx", "head"),
        P("ctx", "head"),
        P("ctx", "head"),
        P("ctx", "head"),
        P("ctx", "head"),
        P("head", "ctx"),
        P("ctx", "head", None),
    )

    step = jax.shard_map(
        local, mesh=mesh, in_specs=placed, out_specs=P("ctx", "head"), check_vma=False
    )
    _, _ = split_ctx(mesh.shape["ctx"], mesh.shape["head"])
    return step
```

```python
import functools
import math

import jax
import jax.numpy as jnp
from jax import lax
from jax.experimental import pallas as pl
from jax.experimental.pallas import tpu as pltpu
from jax.sharding import PartitionSpec as P


BLOCK = 64
HBM = pl.BlockSpec(memory_space=pltpu.HBM)
VMEM = pl.BlockSpec(memory_space=pltpu.VMEM)
SMEM = pl.BlockSpec(memory_space=pltpu.SMEM)
LIMIT = 24 * 1024 * 1024


def split_ctx(devices, head_devices):
    fast = 1
    while (
        (2 * fast) ** 2 <= devices
        and devices % (2 * fast) == 0
        and (devices // (2 * fast)) % head_devices == 0
    ):
        fast *= 2
    return devices // fast, fast


def exchange_tables(selection, blocks_dev, devices):
    groups, heads, picks = selection.shape
    count = groups * heads * picks
    most = (heads * 2 * picks + devices - 1) // devices
    head = lax.broadcasted_iota(jnp.int32, selection.shape, 1)
    owner = (selection // blocks_dev).reshape(count)
    code = ((selection % blocks_dev) * heads + head).reshape(count)
    pair = (selection * heads + head).reshape(count)
    order = jnp.arange(count)
    earlier = order[None, :] < order[:, None]
    same_pair = pair[:, None] == pair[None, :]
    same_owner = owner[:, None] == owner[None, :]
    first = jnp.logical_not(jnp.any(same_pair & earlier, axis=1))
    rank = jnp.sum((same_owner & earlier & first[None, :]).astype(jnp.int32), axis=1)
    slot = jnp.sum(jnp.where(same_pair & first[None, :], rank[None, :], 0), axis=1)
    cell = owner * most + slot
    cells = jnp.arange(devices * most)
    asked = jnp.sum(
        jnp.where((cells[:, None] == cell[None, :]) & first[None, :], code[None, :], 0), axis=1
    )
    return cell, asked.reshape(devices, most)


def gather_kernel(heads, asked_ref, source_ref, out_ref, sem):
    size = out_ref.shape[2]

    def start(cell, carry):
        code = asked_ref[cell]
        row = pl.multiple_of(lax.div(code, heads) * BLOCK, BLOCK)
        column = pl.multiple_of(lax.rem(code, heads) * size, size)
        pltpu.make_async_copy(
            source_ref.at[pl.ds(row, BLOCK), pl.ds(column, size)], out_ref.at[cell], sem
        ).start()
        return carry

    lax.fori_loop(0, out_ref.shape[0], start, 0)
    pltpu.make_async_copy(out_ref, out_ref, sem).wait()


def gather_blocks(asked, source, heads):
    cells = asked.shape[0]
    size = source.shape[1] // heads
    return pl.pallas_call(
        functools.partial(gather_kernel, heads),
        out_shape=jax.ShapeDtypeStruct((cells, BLOCK, size), source.dtype),
        in_specs=[SMEM, HBM],
        out_specs=VMEM,
        scratch_shapes=[pltpu.SemaphoreType.DMA],
        cost_estimate=pl.CostEstimate(
            flops=cells * BLOCK * size * 64,
            bytes_accessed=4 * cells * BLOCK * size,
            transcendentals=0,
        ),
        name="gather_blocks",
    )(asked, source)


def spread_kernel(heads, asked_ref, place_ref, source_ref, *refs):
    outs, sem = refs[:-1], refs[-1]
    most, _, size = outs[0].shape
    for mask, out_ref in enumerate(outs):
        base = (place_ref[3] ^ mask) * most
        for slot in range(most):
            code = asked_ref[base + slot]
            row = pl.multiple_of(lax.div(code, heads) * BLOCK, BLOCK)
            column = pl.multiple_of(lax.rem(code, heads) * size, size)
            pltpu.make_async_copy(
                source_ref.at[pl.ds(row, BLOCK), pl.ds(column, size)],
                out_ref.at[slot],
                sem.at[mask],
            ).start()
    for mask, out_ref in enumerate(outs):
        pltpu.make_async_copy(out_ref, out_ref, sem.at[mask]).wait()


def spread_blocks(asked, place, source, heads, devices):
    most = asked.shape[0] // devices
    size = source.shape[1] // heads
    return pl.pallas_call(
        functools.partial(spread_kernel, heads),
        out_shape=[jax.ShapeDtypeStruct((most, BLOCK, size), source.dtype)] * devices,
        in_specs=[SMEM, SMEM, HBM],
        out_specs=[VMEM] * devices,
        scratch_shapes=[pltpu.SemaphoreType.DMA((devices,))],
        cost_estimate=pl.CostEstimate(
            flops=asked.shape[0] * BLOCK * size * 64,
            bytes_accessed=4 * asked.shape[0] * BLOCK * size,
            transcendentals=0,
        ),
        name="spread_blocks",
    )(asked, place, source)


def fence_kernel(in_ref, out_ref):
    def move(i, carry):
        out_ref[i] = in_ref[i]
        return carry

    lax.fori_loop(0, in_ref.shape[0], move, 0)


def fence(table):
    return pl.pallas_call(
        fence_kernel,
        out_shape=jax.ShapeDtypeStruct(table.shape, table.dtype),
        in_specs=[SMEM],
        out_specs=SMEM,
        name="fence",
    )(table)


def nt_dot(a, b):
    return lax.dot_general(a, b, (((1,), (1,)), ((), ())), preferred_element_type=jnp.float32)


def score_kernel(
    groups, heads, picks, step_heads, cell_ref, q_ref, land_ref, lk_ref, lv_ref, fk_ref,
    weight_ref, acc_ref,
):
    size = q_ref.shape[1] // step_heads
    scaling = 1.0 / math.sqrt(size)
    first_head = pl.program_id(0) * step_heads
    row = lax.broadcasted_iota(jnp.int32, (BLOCK, BLOCK), 0)
    column = lax.broadcasted_iota(jnp.int32, (BLOCK, BLOCK), 1)
    causal = row >= column
    pieces, _, land_rows, _ = land_ref.shape
    chosen = picks * BLOCK
    for hh in range(step_heads):
        cols = slice(hh * size, (hh + 1) * size)
        land_k = land_ref[:, 0, :, cols].reshape(pieces * land_rows, size)
        land_v = land_ref[:, 1, :, cols].reshape(pieces * land_rows, size)
        for g in range(groups):
            rows = slice(g * BLOCK, (g + 1) * BLOCK)
            q = q_ref[rows, cols]
            base = (g * heads + first_head + hh) * picks
            keys = jnp.concatenate([fk_ref[cell_ref[base + p]] for p in range(picks)], axis=0)
            s_land = nt_dot(q, land_k) * scaling
            s_chosen = nt_dot(q, keys) * scaling
            s_local = jnp.where(causal, nt_dot(q, lk_ref[rows, cols]) * scaling, -jnp.inf)
            top = jnp.maximum(
                jnp.maximum(
                    jnp.max(s_land, axis=1, keepdims=True),
                    jnp.max(s_chosen, axis=1, keepdims=True),
                ),
                jnp.max(s_local, axis=1, keepdims=True),
            )
            w_land = jnp.exp(s_land - top)
            w_chosen = jnp.exp(s_chosen - top)
            w_local = jnp.exp(s_local - top)
            total = (
                jnp.sum(w_land, axis=1, keepdims=True)
                + jnp.sum(w_chosen, axis=1, keepdims=True)
                + jnp.sum(w_local, axis=1, keepdims=True)
            )
            inverse = 1.0 / total
            part = jnp.dot(
                w_land.astype(jnp.bfloat16), land_v, preferred_element_type=jnp.float32
            ) + jnp.dot(
                w_local.astype(jnp.bfloat16), lv_ref[rows, cols], preferred_element_type=jnp.float32
            )
            acc_ref[rows, cols] = part * inverse
            weight_ref[rows, hh * chosen : (hh + 1) * chosen] = (w_chosen * inverse).astype(
                jnp.bfloat16
            )


def value_kernel(groups, heads, picks, step_heads, devices, cell_ref, weight_ref, acc_ref, *refs):
    sources, outs, (fv_ref, sem) = refs[:devices], refs[devices:-2], refs[-2:]
    size = acc_ref.shape[1] // step_heads
    most = sources[0].shape[0]

    @pl.when(pl.program_id(0) == 0)
    def _():
        copies = [
            pltpu.make_async_copy(source, fv_ref.at[pl.ds(k * most, most)], sem.at[k])
            for k, source in enumerate(sources)
        ]
        for copy in copies:
            copy.start()
        for copy in copies:
            copy.wait()

    first_head = pl.program_id(0) * step_heads
    chosen = picks * BLOCK
    for hh in range(step_heads):
        cols = slice(hh * size, (hh + 1) * size)
        for g in range(groups):
            rows = slice(g * BLOCK, (g + 1) * BLOCK)
            chunk, inner = divmod(g, groups // len(outs))
            base = (g * heads + first_head + hh) * picks
            values = jnp.concatenate([fv_ref[cell_ref[base + p]] for p in range(picks)], axis=0)
            outs[chunk][inner * BLOCK : (inner + 1) * BLOCK, cols] = (
                acc_ref[rows, cols]
                + jnp.dot(
                    weight_ref[rows, hh * chosen : (hh + 1) * chosen],
                    values,
                    preferred_element_type=jnp.float32,
                )
            ).astype(jnp.bfloat16)


def attention_scores(cell, queries, land, span_keys, span_values, fetched_keys, dims):
    groups, heads, picks = dims
    rows, width = queries.shape
    size = width // heads
    step = math.gcd(heads, 4)
    wide = step * size
    chosen = picks * BLOCK
    by_head = lambda i, c: (0, i)
    keys = land.shape[0] * land.shape[2] + chosen + BLOCK
    return pl.pallas_call(
        functools.partial(score_kernel, groups, heads, picks, step),
        grid_spec=pltpu.PrefetchScalarGridSpec(
            num_scalar_prefetch=1,
            grid=(heads // step,),
            in_specs=[
                pl.BlockSpec((rows, wide), by_head),
                pl.BlockSpec(land.shape[:3] + (wide,), lambda i, c: (0, 0, 0, i)),
                pl.BlockSpec((rows, wide), by_head),
                pl.BlockSpec((rows, wide), by_head),
                pl.BlockSpec(fetched_keys.shape, lambda i, c: (0, 0, 0)),
            ],
            out_specs=[
                pl.BlockSpec((rows, step * chosen), by_head),
                pl.BlockSpec((rows, wide), by_head),
            ],
        ),
        out_shape=[
            jax.ShapeDtypeStruct((rows, heads * chosen), jnp.bfloat16),
            jax.ShapeDtypeStruct((rows, width), jnp.float32),
        ],
        compiler_params=pltpu.CompilerParams(vmem_limit_bytes=LIMIT),
        cost_estimate=pl.CostEstimate(
            flops=16 * rows * keys * width,
            bytes_accessed=16 * rows * width,
            transcendentals=rows * keys * heads,
        ),
        name="attention_scores",
    )(cell, queries, land, span_keys, span_values, fetched_keys)


def attention_values(cell, weights, part, fetched_values, dims):
    groups, heads, picks = dims
    rows, width = part.shape
    devices = len(fetched_values)
    most = fetched_values[0].shape[0]
    size = width // heads
    step = math.gcd(heads, 4)
    wide = step * size
    chosen = picks * BLOCK
    chunks = math.gcd(groups, 2)
    by_head = lambda i, c: (0, i)
    return pl.pallas_call(
        functools.partial(value_kernel, groups, heads, picks, step, devices),
        grid_spec=pltpu.PrefetchScalarGridSpec(
            num_scalar_prefetch=1,
            grid=(heads // step,),
            in_specs=[
                pl.BlockSpec((rows, step * chosen), by_head),
                pl.BlockSpec((rows, wide), by_head),
                *[HBM] * devices,
            ],
            scratch_shapes=[
                pltpu.VMEM((devices * most,) + fetched_values[0].shape[1:], jnp.bfloat16),
                pltpu.SemaphoreType.DMA((devices,)),
            ],
            out_specs=[pl.BlockSpec((rows // chunks, wide), by_head)] * chunks,
        ),
        out_shape=[jax.ShapeDtypeStruct((rows // chunks, width), jnp.bfloat16)] * chunks,
        compiler_params=pltpu.CompilerParams(vmem_limit_bytes=LIMIT),
        cost_estimate=pl.CostEstimate(
            flops=4 * rows * chosen * width,
            bytes_accessed=12 * rows * width,
            transcendentals=0,
        ),
        name="attention_values",
    )(cell, weights, part, *fetched_values)


def pick_kernel(slow_count, head_devices, table, place_ref, *refs):
    b_refs, out_ref, sem = refs[:-2], refs[-2], refs[-1]
    slow, head = place_ref[0], place_ref[1]
    share = slow_count // head_devices
    for slot in range(slow_count):
        target = lax.rem(head + slot // share, head_devices) * share + slot % share
        for step, low, high, members in table:

            @pl.when((target - slow == step) & (slow >= low) & (slow <= high))
            def _():
                row = 0
                for member in members:
                    ref = b_refs[member]
                    rows = pl.ds(row, ref.shape[0])
                    row += ref.shape[0]
                    pltpu.make_async_copy(ref, out_ref.at[slot, rows], sem.at[slot]).start()

    for slot in range(slow_count):
        pltpu.make_async_copy(out_ref.at[slot], out_ref.at[slot], sem.at[slot]).wait()


def pick(place, blocks, slow_count, head_devices):
    arrays, table = [], []
    for step, low, high, chunks in blocks:
        table.append((step, low, high, range(len(arrays), len(arrays) + len(chunks))))
        arrays += chunks
    depth, width = sum(c.shape[0] for c in blocks[0][3]), arrays[0].shape[1]
    return pl.pallas_call(
        functools.partial(pick_kernel, slow_count, head_devices, table),
        out_shape=pltpu.VMEM((slow_count, depth, width), jnp.bfloat16),
        in_specs=[SMEM] + [HBM] * len(arrays),
        out_specs=VMEM,
        scratch_shapes=[pltpu.SemaphoreType.DMA((slow_count,))],
        compiler_params=pltpu.CompilerParams(vmem_limit_bytes=LIMIT // 2),
        cost_estimate=pl.CostEstimate(
            flops=64 * depth * width * slow_count,
            bytes_accessed=4 * depth * width * slow_count,
            transcendentals=0,
        ),
        name="pick",
    )(place, *[pltpu.with_memory_space_constraint(a, pltpu.HBM) for a in arrays])


def project_kernel(share, a_count, *refs):
    a_refs, (b_ref, mine_ref, send_ref) = refs[:a_count], refs[a_count:]
    slots, _, width = b_ref.shape
    for slot in range(slots):
        row = 0
        for a_ref in a_refs:
            rows = slice(row, row + a_ref.shape[0])
            row += a_ref.shape[0]
            product = jnp.dot(a_ref[...], b_ref[slot], preferred_element_type=jnp.float32)
            cols = slice(slot % share * width, (slot % share + 1) * width)
            if slot < share:
                mine_ref[rows, cols] = product
            else:
                send_ref[slot // share - 1, rows, cols] = product.astype(send_ref.dtype)


def project(a_pieces, b_all, share):
    rows = sum(a.shape[0] for a in a_pieces)
    slots, depth, width = b_all.shape
    return pl.pallas_call(
        functools.partial(project_kernel, share, len(a_pieces)),
        out_shape=[
            jax.ShapeDtypeStruct((rows, share * width), jnp.float32),
            jax.ShapeDtypeStruct((slots // share - 1, rows, share * width), jnp.bfloat16),
        ],
        in_specs=[VMEM] * (len(a_pieces) + 1),
        out_specs=[VMEM, VMEM],
        compiler_params=pltpu.CompilerParams(vmem_limit_bytes=LIMIT // 2),
        cost_estimate=pl.CostEstimate(
            flops=2 * rows * depth * width * slots,
            bytes_accessed=2 * depth * width * slots,
            transcendentals=0,
        ),
        name="project",
    )(*a_pieces, b_all)


def assemble_kernel(fast_count, share, others, place_ref, mine_ref, *refs):
    received, tiles, out_ref = refs[:others], refs[others:-1], refs[-1]
    width = mine_ref.shape[1] // share
    for fast in range(fast_count):

        @pl.when(place_ref[2] == fast)
        def _():
            for mask in range(fast_count):
                for block in range(share):
                    cols = slice(block * width, (block + 1) * width)
                    if mask == 0:
                        total = mine_ref[:, cols]
                        for other in received:
                            total = total + other[:, cols].astype(jnp.float32)
                        tile = total.astype(out_ref.dtype)
                    else:
                        tile = tiles[mask - 1][:, cols]
                    start = (block * fast_count + (fast ^ mask)) * width
                    out_ref[:, start : start + width] = tile


def assemble(place, mine, received, tiles, share):
    fast_count = len(tiles) + 1
    rows, wide = mine.shape
    return pl.pallas_call(
        functools.partial(assemble_kernel, fast_count, share, len(received)),
        out_shape=jax.ShapeDtypeStruct((rows, wide * fast_count), jnp.bfloat16),
        in_specs=[SMEM] + [VMEM] * (1 + len(received) + len(tiles)),
        out_specs=VMEM,
        name="assemble",
    )(place, mine, *received, *tiles)


def local(
    queries,
    span_keys,
    span_values,
    cache_keys,
    cache_values,
    land_keys,
    land_values,
    out_weight,
    selection,
):
    _, width = queries.shape
    groups, heads, picks = selection.shape
    size = width // heads
    devices = lax.axis_size("ctx")
    head_devices = lax.axis_size("head")
    slow_count, fast_count = split_ctx(devices, head_devices)
    share = slow_count // head_devices
    bits = [1 << k for k in range(fast_count.bit_length() - 1)]
    index = lax.axis_index("ctx")
    place = jnp.stack(
        [index // fast_count, lax.axis_index("head"), index % fast_count, index]
    )
    place = place.astype(jnp.int32)

    def across(value, mask):
        return lax.ppermute(value, "ctx", [(i, i ^ mask) for i in range(devices)])

    def along(value, shift, low=0, high=None):
        high = slow_count if high is None else high
        pairs = [
            (s * fast_count + f, (s + shift) * fast_count + f)
            for s in range(low, high)
            for f in range(fast_count)
            if 0 <= s + shift < slow_count
        ]
        return lax.ppermute(value, "ctx", pairs)

    blocks_dev = cache_keys.shape[0] // BLOCK
    cell, asked = exchange_tables(selection, blocks_dev, devices)
    asked_for = lax.all_to_all(asked, "ctx", split_axis=0, concat_axis=0, tiled=True)
    asked_for = asked_for.reshape(-1)

    last = slow_count - 1
    blocks = [(0, 0, last, [out_weight])]
    low_parts = high_parts = None
    if slow_count > 1:
        low, high = along(out_weight, 1), along(out_weight, -1)
        blocks += [(-1, 1, last, [low]), (1, 0, last - 1, [high])]
    if slow_count > 2:
        blocks.append((-2, last, last, [along(low, 1, last - 1, last)]))
        blocks.append((2, 0, 0, [along(high, -1, 1, 2)]))
        cut = low.shape[0] // 2
        low_parts, high_parts = [low[:cut], low[cut:]], [high[:cut], high[cut:]]
    land = jnp.stack([land_keys, land_values])[None]
    land_parts = [land]
    for shift in range(1, slow_count):
        pairs = [
            (s * fast_count + f, (s + shift) % slow_count * fast_count + f)
            for s in range(slow_count)
            for f in range(fast_count)
        ]
        land_parts.append(lax.ppermute(land, "ctx", pairs))
    land = jnp.concatenate(land_parts, axis=0)
    for bit in bits:
        land = jnp.concatenate([land, across(land, bit)], axis=0)

    sent = gather_blocks(asked_for, cache_keys, heads).reshape(devices, -1, BLOCK, size)
    got = lax.all_to_all(sent, "ctx", split_axis=0, concat_axis=0, tiled=True)
    fetched_keys = got.reshape(-1, BLOCK, size)
    sent = spread_blocks(asked_for, place, cache_values, heads, devices)
    fetched_values = [sent[0]] + [across(sent[m], m) for m in range(1, devices)]
    cell = fence(cell)
    most = asked.shape[1]
    partner_cell = (cell // most ^ index) * most + cell % most

    dims = (groups, heads, picks)
    weights, part = attention_scores(
        cell, queries, land, span_keys, span_values, fetched_keys, dims
    )
    attended = attention_values(partner_cell, weights, part, fetched_values, dims)

    if slow_count > 3:
        low_parts, high_parts, _ = lax.optimization_barrier(
            (low_parts, high_parts, fetched_values)
        )
    for hop in range(2, slow_count):
        top = last - 1 if hop == 2 else last
        if hop > top:
            break
        for j in range(2):
            low_parts[j] = along(low_parts[j], 1, hop - 1, top)
            high_parts[j] = along(high_parts[j], -1, last - top + 1, last - hop + 2)
        low_parts, high_parts = list(low_parts), list(high_parts)
        blocks.append((-hop, hop, top, list(low_parts)))
        blocks.append((hop, last - top, last - hop, list(high_parts)))

    chunks = len(attended)
    pieces = {0: attended}
    masks = sorted(range(1, fast_count), key=lambda m: (m.bit_count(), m))
    for mask in masks:
        own = [b for b in bits if b & mask]
        pieces[mask] = [None] * chunks
        for j in reversed(range(chunks)) if mask == 1 else range(chunks):
            bit = own[j % len(own)]
            pieces[mask][j] = across(pieces[mask ^ bit][j], bit)

    b_all = pick(place, blocks, slow_count, head_devices)
    tiles = {}
    for mask in [*masks, 0]:
        mine, send = project(pieces[mask], b_all, share)
        received = [
            lax.ppermute(
                send[r - 1], "head", [(h, (h + r) % head_devices) for h in range(head_devices)]
            )
            for r in range(1, head_devices)
        ]
        if mask == 0:
            break
        total = mine
        for other in received:
            total = total + other.astype(jnp.float32)
        tiles[mask] = across(total.astype(jnp.bfloat16), mask)
    return assemble(place, mine, received, [tiles[m] for m in range(1, fast_count)], share)


def solution(mesh):
    placed = (
        P("ctx", "head"),
        P("ctx", "head"),
        P("ctx", "head"),
        P("ctx", "head"),
        P("ctx", "head"),
        P("ctx", "head"),
        P("ctx", "head"),
        P("head", "ctx"),
        P("ctx", "head", None),
    )

    step = jax.shard_map(
        local, mesh=mesh, in_specs=placed, out_specs=P("ctx", "head"), check_vma=False
    )
    _, _ = split_ctx(mesh.shape["ctx"], mesh.shape["head"])
    return step
```

```python
import functools
import math

import jax
import jax.numpy as jnp
from jax import lax
from jax.experimental import pallas as pl
from jax.experimental.pallas import tpu as pltpu
from jax.sharding import PartitionSpec as P


BLOCK = 64
HBM = pl.BlockSpec(memory_space=pltpu.HBM)
VMEM = pl.BlockSpec(memory_space=pltpu.VMEM)
SMEM = pl.BlockSpec(memory_space=pltpu.SMEM)
LIMIT = 24 * 1024 * 1024


def split_ctx(devices, head_devices):
    fast = 1
    while (
        (2 * fast) ** 2 <= devices
        and devices % (2 * fast) == 0
        and (devices // (2 * fast)) % head_devices == 0
    ):
        fast *= 2
    return devices // fast, fast


def exchange_tables(selection, blocks_dev, devices):
    groups, heads, picks = selection.shape
    count = groups * heads * picks
    most = (heads * 2 * picks + devices - 1) // devices
    head = lax.broadcasted_iota(jnp.int32, selection.shape, 1)
    owner = (selection // blocks_dev).reshape(count)
    code = ((selection % blocks_dev) * heads + head).reshape(count)
    pair = (selection * heads + head).reshape(count)
    order = jnp.arange(count)
    earlier = order[None, :] < order[:, None]
    same_pair = pair[:, None] == pair[None, :]
    same_owner = owner[:, None] == owner[None, :]
    first = jnp.logical_not(jnp.any(same_pair & earlier, axis=1))
    rank = jnp.sum((same_owner & earlier & first[None, :]).astype(jnp.int32), axis=1)
    slot = jnp.sum(jnp.where(same_pair & first[None, :], rank[None, :], 0), axis=1)
    cell = owner * most + slot
    cells = jnp.arange(devices * most)
    asked = jnp.sum(
        jnp.where((cells[:, None] == cell[None, :]) & first[None, :], code[None, :], 0), axis=1
    )
    return cell, asked.reshape(devices, most)


def gather_kernel(heads, asked_ref, source_ref, out_ref, sem):
    size = out_ref.shape[2]

    def start(cell, carry):
        code = asked_ref[cell]
        row = pl.multiple_of(lax.div(code, heads) * BLOCK, BLOCK)
        column = pl.multiple_of(lax.rem(code, heads) * size, size)
        pltpu.make_async_copy(
            source_ref.at[pl.ds(row, BLOCK), pl.ds(column, size)], out_ref.at[cell], sem
        ).start()
        return carry

    lax.fori_loop(0, out_ref.shape[0], start, 0)
    pltpu.make_async_copy(out_ref, out_ref, sem).wait()


def gather_blocks(asked, source, heads):
    cells = asked.shape[0]
    size = source.shape[1] // heads
    return pl.pallas_call(
        functools.partial(gather_kernel, heads),
        out_shape=jax.ShapeDtypeStruct((cells, BLOCK, size), source.dtype),
        in_specs=[SMEM, HBM],
        out_specs=VMEM,
        scratch_shapes=[pltpu.SemaphoreType.DMA],
        cost_estimate=pl.CostEstimate(
            flops=cells * BLOCK * size * 64,
            bytes_accessed=4 * cells * BLOCK * size,
            transcendentals=0,
        ),
        name="gather_blocks",
    )(asked, source)


def spread_kernel(heads, asked_ref, place_ref, source_ref, *refs):
    outs, sem = refs[:-1], refs[-1]
    most, _, size = outs[0].shape
    for mask, out_ref in enumerate(outs):
        base = (place_ref[3] ^ mask) * most
        for slot in range(most):
            code = asked_ref[base + slot]
            row = pl.multiple_of(lax.div(code, heads) * BLOCK, BLOCK)
            column = pl.multiple_of(lax.rem(code, heads) * size, size)
            pltpu.make_async_copy(
                source_ref.at[pl.ds(row, BLOCK), pl.ds(column, size)],
                out_ref.at[slot],
                sem.at[mask],
            ).start()
    for mask, out_ref in enumerate(outs):
        pltpu.make_async_copy(out_ref, out_ref, sem.at[mask]).wait()


def spread_blocks(asked, place, source, heads, devices):
    most = asked.shape[0] // devices
    size = source.shape[1] // heads
    return pl.pallas_call(
        functools.partial(spread_kernel, heads),
        out_shape=[jax.ShapeDtypeStruct((most, BLOCK, size), source.dtype)] * devices,
        in_specs=[SMEM, SMEM, HBM],
        out_specs=[VMEM] * devices,
        scratch_shapes=[pltpu.SemaphoreType.DMA((devices,))],
        cost_estimate=pl.CostEstimate(
            flops=asked.shape[0] * BLOCK * size * 64,
            bytes_accessed=4 * asked.shape[0] * BLOCK * size,
            transcendentals=0,
        ),
        name="spread_blocks",
    )(asked, place, source)


def nt_dot(a, b):
    return lax.dot_general(a, b, (((1,), (1,)), ((), ())), preferred_element_type=jnp.float32)


def near_kernel(groups, step_heads, q_ref, land_ref, lk_ref, lv_ref, acc_ref, stat_ref):
    rows = q_ref.shape[0]
    size = q_ref.shape[1] // step_heads
    scaling = 1.0 / math.sqrt(size)
    row = lax.broadcasted_iota(jnp.int32, (rows, BLOCK), 0)
    column = lax.broadcasted_iota(jnp.int32, (rows, BLOCK), 1)
    causal = lax.rem(row, BLOCK) >= column
    spans = [slice(g * BLOCK, (g + 1) * BLOCK) for g in range(groups)]
    pieces, _, land_rows, _ = land_ref.shape
    for hh in range(step_heads):
        cols = slice(hh * size, (hh + 1) * size)
        land_k = land_ref[:, 0, :, cols].reshape(pieces * land_rows, size)
        land_v = land_ref[:, 1, :, cols].reshape(pieces * land_rows, size)
        s_land = nt_dot(q_ref[:, cols], land_k) * scaling
        s_local = jnp.concatenate([nt_dot(q_ref[g, cols], lk_ref[g, cols]) for g in spans], axis=0)
        s_local = jnp.where(causal, s_local * scaling, -jnp.inf)
        top = jnp.maximum(
            jnp.max(s_land, axis=1, keepdims=True), jnp.max(s_local, axis=1, keepdims=True)
        )
        w_land = jnp.exp(s_land - top)
        w_local = jnp.exp(s_local - top)
        stat_ref[hh, :, 0:1] = top
        stat_ref[hh, :, 1:2] = jnp.sum(w_land, axis=1, keepdims=True) + jnp.sum(
            w_local, axis=1, keepdims=True
        )
        w_local = w_local.astype(jnp.bfloat16)
        acc_ref[:, cols] = jnp.dot(
            w_land.astype(jnp.bfloat16), land_v, preferred_element_type=jnp.float32
        ) + jnp.concatenate(
            [
                jnp.dot(w_local[g], lv_ref[g, cols], preferred_element_type=jnp.float32)
                for g in spans
            ],
            axis=0,
        )


def score_kernel(
    groups, heads, picks, step_heads, cell_ref, q_ref, fk_ref, near_ref, stat_ref, weight_ref,
    acc_ref,
):
    size = q_ref.shape[1] // step_heads
    scaling = 1.0 / math.sqrt(size)
    first_head = pl.program_id(0) * step_heads
    chosen = picks * BLOCK
    for hh in range(step_heads):
        cols = slice(hh * size, (hh + 1) * size)
        scores = []
        for g in range(groups):
            base = (g * heads + first_head + hh) * picks
            keys = jnp.concatenate([fk_ref[cell_ref[base + p]] for p in range(picks)], axis=0)
            scores.append(nt_dot(q_ref[g * BLOCK : (g + 1) * BLOCK, cols], keys))
        scores = jnp.concatenate(scores, axis=0) * scaling
        near_top = stat_ref[hh, :, 0:1]
        top = jnp.maximum(near_top, jnp.max(scores, axis=1, keepdims=True))
        weights = jnp.exp(scores - top)
        factor = jnp.exp(near_top - top)
        total = stat_ref[hh, :, 1:2] * factor + jnp.sum(weights, axis=1, keepdims=True)
        inverse = 1.0 / total
        weight_ref[:, hh * chosen : (hh + 1) * chosen] = (weights * inverse).astype(jnp.bfloat16)
        acc_ref[:, cols] = near_ref[:, cols] * (factor * inverse)


def value_kernel(groups, heads, picks, step_heads, devices, cell_ref, weight_ref, acc_ref, *refs):
    sources, outs, (fv_ref, sem) = refs[:devices], refs[devices:-2], refs[-2:]
    size = acc_ref.shape[1] // step_heads
    most = sources[0].shape[0]

    @pl.when(pl.program_id(0) == 0)
    def _():
        copies = [
            pltpu.make_async_copy(source, fv_ref.at[pl.ds(k * most, most)], sem.at[k])
            for k, source in enumerate(sources)
        ]
        for copy in copies:
            copy.start()
        for copy in copies:
            copy.wait()

    first_head = pl.program_id(0) * step_heads
    chosen = picks * BLOCK
    for hh in range(step_heads):
        cols = slice(hh * size, (hh + 1) * size)
        for g in range(groups):
            rows = slice(g * BLOCK, (g + 1) * BLOCK)
            chunk, inner = divmod(g, groups // len(outs))
            base = (g * heads + first_head + hh) * picks
            values = jnp.concatenate([fv_ref[cell_ref[base + p]] for p in range(picks)], axis=0)
            outs[chunk][inner * BLOCK : (inner + 1) * BLOCK, cols] = (
                acc_ref[rows, cols]
                + jnp.dot(
                    weight_ref[rows, hh * chosen : (hh + 1) * chosen],
                    values,
                    preferred_element_type=jnp.float32,
                )
            ).astype(jnp.bfloat16)


def in_hbm(value):
    return pltpu.with_memory_space_constraint(value, pltpu.HBM)


def attention_near(queries, land, span_keys, span_values, dims):
    groups, heads, _ = dims
    rows, width = queries.shape
    size = width // heads
    step = math.gcd(heads, 4)
    wide = step * size
    by_head = lambda i: (0, i)
    keys = land.shape[0] * land.shape[2] + BLOCK
    return pl.pallas_call(
        functools.partial(near_kernel, groups, step),
        grid=(heads // step,),
        in_specs=[
            pl.BlockSpec((rows, wide), by_head),
            pl.BlockSpec(land.shape[:3] + (wide,), lambda i: (0, 0, 0, i)),
            pl.BlockSpec((rows, wide), by_head),
            pl.BlockSpec((rows, wide), by_head),
        ],
        out_specs=[
            pl.BlockSpec((rows, wide), by_head),
            pl.BlockSpec((step, rows, 2), lambda i: (i, 0, 0)),
        ],
        out_shape=[
            jax.ShapeDtypeStruct((rows, width), jnp.float32),
            jax.ShapeDtypeStruct((heads, rows, 2), jnp.float32),
        ],
        compiler_params=pltpu.CompilerParams(vmem_limit_bytes=LIMIT),
        cost_estimate=pl.CostEstimate(
            flops=16 * rows * keys * width,
            bytes_accessed=16 * rows * width,
            transcendentals=rows * keys * heads,
        ),
        name="attention_near",
    )(in_hbm(queries), in_hbm(land), in_hbm(span_keys), in_hbm(span_values))


def attention_scores(cell, queries, fetched_keys, near, stats, dims):
    groups, heads, picks = dims
    rows, width = queries.shape
    size = width // heads
    step = math.gcd(heads, 4)
    wide = step * size
    chosen = picks * BLOCK
    by_head = lambda i, c: (0, i)
    return pl.pallas_call(
        functools.partial(score_kernel, groups, heads, picks, step),
        grid_spec=pltpu.PrefetchScalarGridSpec(
            num_scalar_prefetch=1,
            grid=(heads // step,),
            in_specs=[
                pl.BlockSpec((rows, wide), by_head),
                pl.BlockSpec(fetched_keys.shape, lambda i, c: (0, 0, 0)),
                pl.BlockSpec((rows, wide), by_head),
                pl.BlockSpec((step, rows, 2), lambda i, c: (i, 0, 0)),
            ],
            out_specs=[
                pl.BlockSpec((rows, step * chosen), by_head),
                pl.BlockSpec((rows, wide), by_head),
            ],
        ),
        out_shape=[
            pltpu.VMEM((rows, heads * chosen), jnp.bfloat16),
            pltpu.VMEM((rows, width), jnp.float32),
        ],
        compiler_params=pltpu.CompilerParams(vmem_limit_bytes=LIMIT),
        cost_estimate=pl.CostEstimate(
            flops=8 * rows * chosen * width,
            bytes_accessed=16 * rows * width,
            transcendentals=rows * chosen * heads,
        ),
        name="attention_scores",
    )(cell, in_hbm(queries), fetched_keys, in_hbm(near), in_hbm(stats))


def attention_values(cell, weights, part, fetched_values, dims):
    groups, heads, picks = dims
    rows, width = part.shape
    devices = len(fetched_values)
    most = fetched_values[0].shape[0]
    size = width // heads
    step = math.gcd(heads, 4)
    wide = step * size
    chosen = picks * BLOCK
    chunks = math.gcd(groups, 2)
    by_head = lambda i, c: (0, i)
    return pl.pallas_call(
        functools.partial(value_kernel, groups, heads, picks, step, devices),
        grid_spec=pltpu.PrefetchScalarGridSpec(
            num_scalar_prefetch=1,
            grid=(heads // step,),
            in_specs=[
                pl.BlockSpec((rows, step * chosen), by_head),
                pl.BlockSpec((rows, wide), by_head),
                *[HBM] * devices,
            ],
            scratch_shapes=[
                pltpu.VMEM((devices * most,) + fetched_values[0].shape[1:], jnp.bfloat16),
                pltpu.SemaphoreType.DMA((devices,)),
            ],
            out_specs=[pl.BlockSpec((rows // chunks, wide), by_head)] * chunks,
        ),
        out_shape=[jax.ShapeDtypeStruct((rows // chunks, width), jnp.bfloat16)] * chunks,
        compiler_params=pltpu.CompilerParams(vmem_limit_bytes=LIMIT),
        cost_estimate=pl.CostEstimate(
            flops=4 * rows * chosen * width,
            bytes_accessed=12 * rows * width,
            transcendentals=0,
        ),
        name="attention_values",
    )(cell, weights, part, *fetched_values)


def pick_kernel(slow_count, head_devices, table, place_ref, *refs):
    b_refs, out_ref, sem = refs[:-2], refs[-2], refs[-1]
    slow, head = place_ref[0], place_ref[1]
    share = slow_count // head_devices
    for slot in range(slow_count):
        target = lax.rem(head + slot // share, head_devices) * share + slot % share
        for step, low, high, members in table:

            @pl.when((target - slow == step) & (slow >= low) & (slow <= high))
            def _():
                row = 0
                for member in members:
                    ref = b_refs[member]
                    rows = pl.ds(row, ref.shape[0])
                    row += ref.shape[0]
                    pltpu.make_async_copy(ref, out_ref.at[slot, rows], sem.at[slot]).start()

    for slot in range(slow_count):
        pltpu.make_async_copy(out_ref.at[slot], out_ref.at[slot], sem.at[slot]).wait()


def pick(place, blocks, slow_count, head_devices):
    arrays, table = [], []
    for step, low, high, chunks in blocks:
        table.append((step, low, high, range(len(arrays), len(arrays) + len(chunks))))
        arrays += chunks
    depth, width = sum(c.shape[0] for c in blocks[0][3]), arrays[0].shape[1]
    return pl.pallas_call(
        functools.partial(pick_kernel, slow_count, head_devices, table),
        out_shape=pltpu.VMEM((slow_count, depth, width), jnp.bfloat16),
        in_specs=[SMEM] + [HBM] * len(arrays),
        out_specs=VMEM,
        scratch_shapes=[pltpu.SemaphoreType.DMA((slow_count,))],
        compiler_params=pltpu.CompilerParams(vmem_limit_bytes=LIMIT // 2),
        cost_estimate=pl.CostEstimate(
            flops=64 * depth * width * slow_count,
            bytes_accessed=4 * depth * width * slow_count,
            transcendentals=0,
        ),
        name="pick",
    )(place, *[pltpu.with_memory_space_constraint(a, pltpu.HBM) for a in arrays])


def project_kernel(share, a_count, *refs):
    a_refs, (b_ref, mine_ref, send_ref) = refs[:a_count], refs[a_count:]
    slots, _, width = b_ref.shape
    for slot in range(slots):
        row = 0
        for a_ref in a_refs:
            rows = slice(row, row + a_ref.shape[0])
            row += a_ref.shape[0]
            product = jnp.dot(a_ref[...], b_ref[slot], preferred_element_type=jnp.float32)
            cols = slice(slot % share * width, (slot % share + 1) * width)
            if slot < share:
                mine_ref[rows, cols] = product
            else:
                send_ref[slot // share - 1, rows, cols] = product.astype(send_ref.dtype)


def project(a_pieces, b_all, share):
    rows = sum(a.shape[0] for a in a_pieces)
    slots, depth, width = b_all.shape
    return pl.pallas_call(
        functools.partial(project_kernel, share, len(a_pieces)),
        out_shape=[
            jax.ShapeDtypeStruct((rows, share * width), jnp.float32),
            jax.ShapeDtypeStruct((slots // share - 1, rows, share * width), jnp.bfloat16),
        ],
        in_specs=[VMEM] * (len(a_pieces) + 1),
        out_specs=[VMEM, VMEM],
        compiler_params=pltpu.CompilerParams(vmem_limit_bytes=LIMIT // 2),
        cost_estimate=pl.CostEstimate(
            flops=2 * rows * depth * width * slots,
            bytes_accessed=2 * depth * width * slots,
            transcendentals=0,
        ),
        name="project",
    )(*a_pieces, b_all)


def assemble_kernel(fast_count, share, others, place_ref, mine_ref, *refs):
    received, tiles, out_ref = refs[:others], refs[others:-1], refs[-1]
    width = mine_ref.shape[1] // share
    for fast in range(fast_count):

        @pl.when(place_ref[2] == fast)
        def _():
            for mask in range(fast_count):
                for block in range(share):
                    cols = slice(block * width, (block + 1) * width)
                    if mask == 0:
                        total = mine_ref[:, cols]
                        for other in received:
                            total = total + other[:, cols].astype(jnp.float32)
                        tile = total.astype(out_ref.dtype)
                    else:
                        tile = tiles[mask - 1][:, cols]
                    start = (block * fast_count + (fast ^ mask)) * width
                    out_ref[:, start : start + width] = tile


def assemble(place, mine, received, tiles, share):
    fast_count = len(tiles) + 1
    rows, wide = mine.shape
    return pl.pallas_call(
        functools.partial(assemble_kernel, fast_count, share, len(received)),
        out_shape=jax.ShapeDtypeStruct((rows, wide * fast_count), jnp.bfloat16),
        in_specs=[SMEM] + [VMEM] * (1 + len(received) + len(tiles)),
        out_specs=VMEM,
        name="assemble",
    )(place, mine, *received, *tiles)


def local(
    queries,
    span_keys,
    span_values,
    cache_keys,
    cache_values,
    land_keys,
    land_values,
    out_weight,
    selection,
):
    _, width = queries.shape
    groups, heads, picks = selection.shape
    size = width // heads
    devices = lax.axis_size("ctx")
    head_devices = lax.axis_size("head")
    slow_count, fast_count = split_ctx(devices, head_devices)
    share = slow_count // head_devices
    bits = [1 << k for k in range(fast_count.bit_length() - 1)]
    index = lax.axis_index("ctx")
    place = jnp.stack(
        [index // fast_count, lax.axis_index("head"), index % fast_count, index]
    )
    place = place.astype(jnp.int32)

    def across(value, mask):
        return lax.ppermute(value, "ctx", [(i, i ^ mask) for i in range(devices)])

    def along(value, shift, low=0, high=None):
        high = slow_count if high is None else high
        pairs = [
            (s * fast_count + f, (s + shift) * fast_count + f)
            for s in range(low, high)
            for f in range(fast_count)
            if 0 <= s + shift < slow_count
        ]
        return lax.ppermute(value, "ctx", pairs)

    blocks_dev = cache_keys.shape[0] // BLOCK
    cell, asked = exchange_tables(selection, blocks_dev, devices)
    asked_for = lax.all_to_all(asked, "ctx", split_axis=0, concat_axis=0, tiled=True)
    asked_for = asked_for.reshape(-1)

    last = slow_count - 1
    blocks = [(0, 0, last, [out_weight])]
    low_parts = high_parts = None
    if slow_count > 1:
        low, high = along(out_weight, 1), along(out_weight, -1)
        blocks += [(-1, 1, last, [low]), (1, 0, last - 1, [high])]
    if slow_count > 2:
        blocks.append((-2, last, last, [along(low, 1, last - 1, last)]))
        blocks.append((2, 0, 0, [along(high, -1, 1, 2)]))
        cut = low.shape[0] // 2
        low_parts, high_parts = [low[:cut], low[cut:]], [high[:cut], high[cut:]]
    land = jnp.stack([land_keys, land_values])[None]
    land_parts = [land]
    for shift in range(1, slow_count):
        pairs = [
            (s * fast_count + f, (s + shift) % slow_count * fast_count + f)
            for s in range(slow_count)
            for f in range(fast_count)
        ]
        land_parts.append(lax.ppermute(land, "ctx", pairs))
    land = jnp.concatenate(land_parts, axis=0)
    for bit in bits:
        land = jnp.concatenate([land, across(land, bit)], axis=0)

    sent = gather_blocks(asked_for, cache_keys, heads).reshape(devices, -1, BLOCK, size)
    got = lax.all_to_all(sent, "ctx", split_axis=0, concat_axis=0, tiled=True)
    fetched_keys = got.reshape(-1, BLOCK, size)
    sent = spread_blocks(asked_for, place, cache_values, heads, devices)
    fetched_values = [sent[0]] + [across(sent[m], m) for m in range(1, devices)]
    most = asked.shape[1]
    partner_cell = (cell // most ^ index) * most + cell % most

    dims = (groups, heads, picks)
    near, stats = attention_near(queries, land, span_keys, span_values, dims)
    weights, part = attention_scores(cell, queries, fetched_keys, near, stats, dims)
    attended = attention_values(partner_cell, weights, part, fetched_values, dims)

    for hop in range(2, slow_count):
        top = last - 1 if hop == 2 else last
        if hop > top:
            break
        for j in range(2):
            low_parts[j] = along(low_parts[j], 1, hop - 1, top)
            high_parts[j] = along(high_parts[j], -1, last - top + 1, last - hop + 2)
        low_parts, high_parts = list(low_parts), list(high_parts)
        blocks.append((-hop, hop, top, list(low_parts)))
        blocks.append((hop, last - top, last - hop, list(high_parts)))

    chunks = len(attended)
    pieces = {0: attended}
    masks = sorted(range(1, fast_count), key=lambda m: (m.bit_count(), m))
    for mask in masks:
        own = [b for b in bits if b & mask]
        pieces[mask] = [None] * chunks
        for j in reversed(range(chunks)) if mask == 1 else range(chunks):
            bit = own[j % len(own)]
            pieces[mask][j] = across(pieces[mask ^ bit][j], bit)

    b_all = pick(place, blocks, slow_count, head_devices)
    tiles = {}
    for mask in [*reversed(masks), 0]:
        mine, send = project(pieces[mask], b_all, share)
        received = [
            lax.ppermute(
                send[r - 1], "head", [(h, (h + r) % head_devices) for h in range(head_devices)]
            )
            for r in range(1, head_devices)
        ]
        if mask == 0:
            break
        total = mine
        for other in received:
            total = total + other.astype(jnp.float32)
        tiles[mask] = across(total.astype(jnp.bfloat16), mask)
    return assemble(place, mine, received, [tiles[m] for m in range(1, fast_count)], share)


def solution(mesh):
    placed = (
        P("ctx", "head"),
        P("ctx", "head"),
        P("ctx", "head"),
        P("ctx", "head"),
        P("ctx", "head"),
        P("ctx", "head"),
        P("ctx", "head"),
        P("head", "ctx"),
        P("ctx", "head", None),
    )

    step = jax.shard_map(
        local, mesh=mesh, in_specs=placed, out_specs=P("ctx", "head"), check_vma=False
    )
    _, _ = split_ctx(mesh.shape["ctx"], mesh.shape["head"])
    return step
```
